256 devices in a mesh: rows: 64 (over x, y, z_lo), rep: 4 (over z_hi, core).
Axes of the slice: x: 4, y: 4, z: 8 (z_hi: 2, z_lo: 4; z = z_hi * 4 + z_lo), core: 2. Of those that a mesh axis runs over, the one named last changes fastest.
Arguments:
- x_tiles: bfloat16 [512, 10, 128, 128], P('rows'), may hold values from -2.5 to 2.5
- giant_tiles: bfloat16 [512, 10, 128, 128], P('rows'), may hold values from -2.5 to 2.5
- coeffs: float32 [3], replicated, may hold values from 0.5 to 1.5
- pattern: int32 [512, 10], replicated, may hold values from 0 to 511, as said below
Outputs:
- squared: bfloat16 [512, 10, 128, 128], P('rows')
- result: bfloat16 [512, 10, 128, 128], P('rows')
The draws below stay inside these ranges and needn't reach their ends.
Inputs may be any that keep to these rules, and one draw needn't show every extreme that they name: `pattern`: slots 2 j and 2 j + 1 of block row i hold two different tile columns of panel (i // 8 + j - 2) mod (64), a panel being 8 consecutive block rows, for j = 0 to 4; slot 4 holds i itself.
All inputs are finite; a program needn't handle non-finite values.
Results may differ from the reference program's by a relative error of at most 0.012.
Values may be sent and summed in bfloat16 or wider, within the bound.
A program may use at most 128 MiB of HBM per device.

```python
import jax
import jax.numpy as jnp
from jax import lax

TILE = 128
RB = 8
HALF = 2
KP = 2
K = 10
NB = 512


def draw_pattern(key, part):
    panel_count = NB // RB
    block_rows = jnp.arange(NB, dtype=jnp.int32)
    home = block_rows // RB
    within = block_rows % RB
    spread = 2 * HALF + 1
    first_key, second_key = jax.random.split(jax.random.fold_in(key, 17))
    first = jax.random.randint(first_key, (NB, spread), 0, RB, dtype=jnp.int32)
    first = jnp.where(jnp.arange(spread, dtype=jnp.int32)[None, :] == HALF, within[:, None], first)
    second = (first + jax.random.randint(second_key, (NB, spread), 1, RB, dtype=jnp.int32)) % RB
    panel = (home[:, None] + jnp.arange(spread, dtype=jnp.int32)[None, :] - HALF) % panel_count
    both = jnp.stack([panel * RB + first, panel * RB + second], axis=-1)
    return both.reshape(NB, spread * 2).astype(jnp.int32)


def block_scale(key, dims, cuts, smallest, top_value):
    gain, own = 1.0, jax.random.fold_in(key, 6)
    for position, shards_of in cuts:
        steps = jnp.exp(jax.random.uniform(jax.random.fold_in(own, position), (shards_of,), jnp.float32, smallest / len(cuts), top_value / len(cuts)))
        gain = gain * jnp.repeat(steps, dims[position] // shards_of).reshape([-1 if axis == position else 1 for axis in range(len(dims))])
    return gain


def gaussian(key, dims, deviation, most, cuts=(), kind=jnp.bfloat16):
    drawn = jax.random.normal(key, dims, jnp.float32) * deviation
    if len(cuts) > 0:
        drawn = block_scale(key, dims, cuts, -0.22, 0.18) * drawn
    return jnp.clip(drawn, min=-most, max=most).astype(kind)


def setup_inputs(seed: int = 0) -> dict:
    key_list = jax.random.split(jax.random.key(seed), 5)
    return {
        "x_tiles": gaussian(key_list[0], (NB, K, TILE, TILE), (2.0 / TILE ** 0.5), 2.5, ((0, 64),)),
        "giant_tiles": gaussian(key_list[1], (NB, K, TILE, TILE), (2.0 / TILE ** 0.5), 2.5, ((0, 64),)),
        "coeffs": jnp.clip(jax.random.uniform(key_list[2], (3,), jnp.float32, 0.5, 1.5), 0.5, 1.5),
        "pattern": draw_pattern(jax.random.fold_in(key_list[4], 71), 0),
    }


def truncated(left, right, pattern):
    def one_row(index):
        columns = pattern[index]
        left_row = left[index].astype(jnp.float32)
        right_rows = right[columns].astype(jnp.float32)
        right_cols = pattern[columns]
        matches = (right_cols[:, :, None] == columns[None, None, :]).astype(jnp.float32)
        chosen = jnp.einsum('stu,stxy->suxy', matches, right_rows, precision=lax.Precision.HIGHEST)
        return jnp.einsum('sxz,suzy->uxy', left_row, chosen, precision=lax.Precision.HIGHEST)

    return lax.map(one_row, jnp.arange(NB, dtype=jnp.int32))


def reference(x_tiles, giant_tiles, coeffs, pattern):
    squared = truncated(x_tiles, x_tiles, pattern).astype(jnp.bfloat16)
    diagonal_slot = (jnp.arange(K, dtype=jnp.int32) == HALF * KP).astype(jnp.float32)
    identity = diagonal_slot[:, None, None] * jnp.eye(TILE, dtype=jnp.float32)[None, :, :]
    baby = coeffs[0] * identity[None] + coeffs[1] * x_tiles.astype(jnp.float32) + coeffs[2] * squared.astype(jnp.float32)
    baby = baby.astype(jnp.bfloat16)
    result = truncated(giant_tiles, baby, pattern).astype(jnp.bfloat16)
    return squared, result
```

```python
import functools

import jax
import jax.numpy as jnp
from jax import lax
from jax.experimental import pallas as pl
from jax.experimental.pallas import tpu as pltpu
from jax.sharding import PartitionSpec as P

HALF = 2
KP = 2
SPREAD = 2 * HALF + 1
UNROLL = 4
MESH = pl.DeviceIdType.MESH

ORDER = (
    ((1, 1), (1, 0), (1, -1), (1, 2), (2, 2), (2, 1), (2, 0)),
    ((1, -1), (1, 0), (1, 2), (1, 1), (2, 0), (2, 1), (2, 2)),
)
NEAR = 4
GROUPS = len(ORDER[0])


def kernel(panels, run, copies, pat, coef, x_hbm, g_hbm, squared_hbm, result_hbm, *scratch):
    (xv, gv, bv, sv, rv, acc, near0, near1, far0, far1, load_sem, out_sem, send_sem, recv_sem, push_sem, pull_sem) = _unpack(scratch)
    rows = xv.shape[0]
    side = xv.shape[2]
    half = rows // 2
    panel = lax.axis_index("rows")
    rep = lax.axis_index("rep")
    core = rep % 2
    zone = rep // 2
    place = panel % run
    if copies > 1:
        zone_up = jnp.where(place == run - 1, 1 - zone, zone)
        zone_down = jnp.where(place == 0, 1 - zone, zone)
    else:
        zone_up = zone
        zone_down = zone
    above = ((panel + 1) % panels, zone_up * 2 + core)
    below = ((panel + panels - 1) % panels, zone_down * 2 + core)
    partner = (panel, zone * 2 + 1 - core)

    loads = [pltpu.make_async_copy(x_hbm, xv, load_sem.at[0]), pltpu.make_async_copy(g_hbm, gv, load_sem.at[1])]
    for load in loads:
        load.start()

    barrier = pltpu.get_barrier_semaphore()
    for other in (above, below, partner):
        pl.semaphore_signal(barrier, inc=1, device_id=other, device_id_type=MESH)
    pl.semaphore_wait(barrier, 3)

    near = (near0, near1)
    far = (far0, far1)
    mine = (xv, bv)
    my_half = pl.ds(core * half, half)
    sends = []

    def landing(phase, group):
        return near[phase][group] if group < NEAR else far[phase][group - NEAR]

    def hop(phase, group, end):
        distance, column = ORDER[phase][group]
        sign = 1 - 2 * end
        slots = sign * (column - distance) + HALF
        if distance == 1:
            source = mine[phase].at[my_half, pl.ds(slots * KP, KP)]
        else:
            source = landing(phase, ORDER[phase].index((1, column - 1))).at[end, my_half]
        index = (phase * GROUPS + group) * 2 + end
        return pltpu.make_async_remote_copy(
            src_ref=source,
            dst_ref=landing(phase, group).at[end, my_half],
            send_sem=send_sem.at[index],
            recv_sem=recv_sem.at[index],
            device_id=above if end else below,
            device_id_type=MESH,
        )

    def push(phase, group, end):
        index = (phase * GROUPS + group) * 2 + end
        block = landing(phase, group).at[end, my_half]
        return pltpu.make_async_remote_copy(
            src_ref=block,
            dst_ref=block,
            send_sem=push_sem.at[index],
            recv_sem=pull_sem.at[index],
            device_id=partner,
            device_id_type=MESH,
        )

    def start(phase, group):
        for end in (0, 1):
            copy = hop(phase, group, end)
            copy.start()
            sends.append(copy)

    def arrive(phase, group):
        for end in (0, 1):
            hop(phase, group, end).wait_recv()
        distance, column = ORDER[phase][group]
        if (distance + 1, column + 1) in ORDER[phase]:
            start(phase, ORDER[phase].index((distance + 1, column + 1)))
        for end in (0, 1):
            copy = push(phase, group, end)
            copy.start()
            sends.append(copy)
        for end in (0, 1):
            push(phase, group, end).wait_recv()

    def term(left, i, distance, column, tile_at):
        at = (panel * rows + i) * (SPREAD * KP)
        first = (distance + HALF) * KP
        wanted = (column + HALF) * KP
        offered = (column - distance + HALF) * KP
        columns = [pat[at + wanted + u] for u in range(KP)]
        deep = []
        for s in range(KP):
            k = pat[at + first + s]
            held = [pat[k * (SPREAD * KP) + offered + t] for t in range(KP)]
            wide = []
            for u in range(KP):
                second = held[1] == columns[u]
                found = jnp.logical_or(held[0] == columns[u], second)
                tile = tile_at(k % rows, jnp.where(second, 1, 0))
                wide.append(jnp.where(found, tile, jnp.zeros_like(tile)))
            deep.append(jnp.concatenate(wide, axis=1))
        weights = jnp.concatenate(deep, axis=0)
        factor = jnp.concatenate([left[i, first], left[i, first + 1]], axis=1)
        return jnp.dot(factor, weights, preferred_element_type=jnp.float32)

    def own_terms(left, right, column):
        def step(n, carry):
            for q in range(UNROLL):
                i = n * UNROLL + q
                acc[column + HALF, i] = term(left, i, 0, column, lambda r, t: right[r, (column + HALF) * KP + t])
            return carry

        lax.fori_loop(0, rows // UNROLL, step, 0)

    def group_terms(left, phase, group):
        distance, column = ORDER[phase][group]
        buffer = landing(phase, group)
        per = rows // UNROLL

        def step(n, carry):
            end = n // per
            sign = 1 - 2 * end
            for q in range(UNROLL):
                i = (n % per) * UNROLL + q
                here = sign * column
                acc[here + HALF, i] += term(left, i, sign * distance, here, lambda r, t: buffer[end, r, t])
            return carry

        lax.fori_loop(0, 2 * per, step, 0)

    def settle(column):
        def step(i, carry):
            total = acc[column + HALF, i]
            for u in range(KP):
                slot = (column + HALF) * KP + u
                tile = total[:, u * side : (u + 1) * side].astype(jnp.bfloat16)
                sv[i, slot] = tile
                mixed = coef[1] * xv[i, slot].astype(jnp.float32) + coef[2] * tile.astype(jnp.float32)
                if slot == HALF * KP:
                    down = lax.broadcasted_iota(jnp.int32, (side, side), 0)
                    across = lax.broadcasted_iota(jnp.int32, (side, side), 1)
                    mixed = mixed + jnp.where(down == across, coef[0], 0.0)
                bv[i, slot] = mixed.astype(jnp.bfloat16)
            return carry

        lax.fori_loop(0, rows, step, 0)
        own_terms(gv, bv, column)
        put(0, column, sv, squared_hbm)

    def put(which, column, source, target):
        slots = pl.ds((column + HALF) * KP, KP)
        copy = pltpu.make_async_copy(source.at[:, slots], target.at[:, slots], out_sem.at[which * SPREAD + column + HALF])
        copy.start()
        outs.append(copy)

    def finish(column):
        def step(i, carry):
            total = acc[column + HALF, i]
            for u in range(KP):
                rv[i, (column + HALF) * KP + u] = total[:, u * side : (u + 1) * side].astype(jnp.bfloat16)
            return carry

        lax.fori_loop(0, rows, step, 0)
        put(1, column, rv, result_hbm)

    outs = []
    loads[0].wait()
    for group in range(NEAR):
        start(0, group)
    for column in range(-HALF, HALF + 1):
        own_terms(xv, xv, column)
    loads[1].wait()
    for group in range(NEAR):
        arrive(0, group)
        group_terms(xv, 0, group)
    arrive(0, 4)
    group_terms(xv, 0, 4)
    settle(2)
    settle(-2)
    start(1, 0)
    arrive(0, 5)
    group_terms(xv, 0, 5)
    settle(1)
    settle(-1)
    start(1, 1)
    start(1, 2)
    arrive(0, 6)
    group_terms(xv, 0, 6)
    settle(0)
    start(1, 3)
    for group in range(NEAR):
        arrive(1, group)
        group_terms(gv, 1, group)
    for group in range(NEAR, GROUPS):
        arrive(1, group)
        group_terms(gv, 1, group)
        column = ORDER[1][group][1]
        finish(column)
        if column:
            finish(-column)
    for copy in outs:
        copy.wait()
    for copy in sends:
        copy.wait_send()


def _unpack(scratch):
    at = 6
    near0, near1 = scratch[at : at + 4], scratch[at + 4 : at + 8]
    far0, far1 = scratch[at + 8 : at + 11], scratch[at + 11 : at + 14]
    return scratch[:6] + (near0, near1, far0, far1) + scratch[at + 14 :]


def solution(mesh):
    panels = mesh.shape["rows"]
    copies = mesh.shape["rep"] // 2

    def local(x_tiles, giant_tiles, coeffs, pattern):
        rows, slots, side, _ = x_tiles.shape
        tiles = pltpu.VMEM(x_tiles.shape, jnp.bfloat16)
        chunk = pltpu.VMEM((2, rows, KP, side, side), jnp.bfloat16)
        moves = 2 * GROUPS * 2
        outs = jax.ShapeDtypeStruct(x_tiles.shape, jnp.bfloat16)
        return pl.pallas_call(
            functools.partial(kernel, panels, 4, copies),
            out_shape=(outs, outs),
            in_specs=[
                pl.BlockSpec(memory_space=pltpu.SMEM),
                pl.BlockSpec(memory_space=pltpu.SMEM),
                pl.BlockSpec(memory_space=pl.ANY),
                pl.BlockSpec(memory_space=pl.ANY),
            ],
            out_specs=(pl.BlockSpec(memory_space=pl.ANY), pl.BlockSpec(memory_space=pl.ANY)),
            scratch_shapes=[
                tiles,
                tiles,
                tiles,
                tiles,
                tiles,
                pltpu.VMEM((SPREAD, rows, side, KP * side), jnp.float32),
                *[chunk for _ in range(2 * GROUPS)],
                pltpu.SemaphoreType.DMA((2,)),
                pltpu.SemaphoreType.DMA((2 * SPREAD,)),
                pltpu.SemaphoreType.DMA((moves,)),
                pltpu.SemaphoreType.DMA((moves,)),
                pltpu.SemaphoreType.DMA((moves,)),
                pltpu.SemaphoreType.DMA((moves,)),
            ],
            compiler_params=pltpu.CompilerParams(
                collective_id=0, has_side_effects=True, vmem_limit_bytes=60 * 1024 * 1024
            ),
        )(pattern.reshape(-1), coeffs, x_tiles, giant_tiles)

    return jax.shard_map(
        local,
        mesh=mesh,
        in_specs=(P("rows", None, None, None), P("rows", None, None, None), P(), P()),
        out_specs=(P("rows", None, None, None), P("rows", None, None, None)),
        check_vma=False,
    )
```

```python
import functools

import jax
import jax.numpy as jnp
from jax import lax
from jax.experimental import pallas as pl
from jax.experimental.pallas import tpu as pltpu
from jax.sharding import PartitionSpec as P

HALF = 2
KP = 2
SPREAD = 2 * HALF + 1
UNROLL = 4
MESH = pl.DeviceIdType.MESH

ORDER = (
    ((1, -1), (1, 0), (1, 1), (1, 2), (2, 0), (2, 1), (2, 2)),
    ((1, 1), (2, 1), (1, 2), (2, 2)),
)
FORMED = ((1, -1), (1, 0), (2, 0))
MOVES = [(phase, group) for phase in (0, 1) for group in ORDER[phase]]


def kernel(panels, run, copies, pat, coef, x_hbm, g_hbm, squared_hbm, result_hbm, *scratch):
    xv, gv, bv, sv, rv, acc = scratch[:6]
    arrived = dict(zip(MOVES, scratch[6:]))
    formed = dict(zip(FORMED, scratch[6 + len(MOVES) :]))
    load_sem, out_sem, send_sem, recv_sem, push_sem, pull_sem = scratch[-6:]
    rows = xv.shape[0]
    side = xv.shape[2]
    half = rows // 2
    panel = lax.axis_index("rows")
    rep = lax.axis_index("rep")
    core = rep % 2
    zone = rep // 2
    place = panel % run
    if copies > 1:
        zone_up = jnp.where(place == run - 1, 1 - zone, zone)
        zone_down = jnp.where(place == 0, 1 - zone, zone)
    else:
        zone_up = zone
        zone_down = zone
    above = ((panel + 1) % panels, zone_up * 2 + core)
    below = ((panel + panels - 1) % panels, zone_down * 2 + core)
    partner = (panel, zone * 2 + 1 - core)

    loads = [pltpu.make_async_copy(x_hbm, xv, load_sem.at[0]), pltpu.make_async_copy(g_hbm, gv, load_sem.at[1])]
    for load in loads:
        load.start()

    barrier = pltpu.get_barrier_semaphore()
    for other in (above, below, partner):
        pl.semaphore_signal(barrier, inc=1, device_id=other, device_id_type=MESH)
    pl.semaphore_wait(barrier, 3)

    mine = (xv, bv)
    my_half = pl.ds(core * half, half)
    sends = []
    outs = []

    def hop(phase, group, end):
        distance, column = group
        if distance == 1:
            slots = (1 - 2 * end) * (column - distance) + HALF
            source = mine[phase].at[my_half, pl.ds(slots * KP, KP)]
        else:
            passed = (distance - 1, column - 1)
            held = formed[passed] if phase and passed in FORMED else arrived[phase, passed]
            source = held.at[end, my_half]
        index = MOVES.index((phase, group)) * 2 + end
        return pltpu.make_async_remote_copy(
            src_ref=source,
            dst_ref=arrived[phase, group].at[end, my_half],
            send_sem=send_sem.at[index],
            recv_sem=recv_sem.at[index],
            device_id=above if end else below,
            device_id_type=MESH,
        )

    def push(phase, group, end):
        index = MOVES.index((phase, group)) * 2 + end
        block = arrived[phase, group].at[end, my_half]
        return pltpu.make_async_remote_copy(
            src_ref=block,
            dst_ref=block,
            send_sem=push_sem.at[index],
            recv_sem=pull_sem.at[index],
            device_id=partner,
            device_id_type=MESH,
        )

    def start(phase, group):
        for end in (0, 1):
            copy = hop(phase, group, end)
            copy.start()
            sends.append(copy)

    def arrive(phase, group, passing=None):
        for end in (0, 1):
            hop(phase, group, end).wait_recv()
        if passing:
            start(phase, passing)
        for end in (0, 1):
            copy = push(phase, group, end)
            copy.start()
            sends.append(copy)
        for end in (0, 1):
            push(phase, group, end).wait_recv()

    def term(i, row, middle, column, left_at, right_at):
        at = ((panel + row + panels) % panels * rows + i) * (SPREAD * KP)
        first = (middle - row + HALF) * KP
        wanted = (column - row + HALF) * KP
        offered = (column - middle + HALF) * KP
        columns = [pat[at + wanted + u] for u in range(KP)]
        deep = []
        for s in range(KP):
            k = pat[at + first + s]
            held = [pat[k * (SPREAD * KP) + offered + t] for t in range(KP)]
            wide = []
            for u in range(KP):
                second = held[1] == columns[u]
                found = jnp.logical_or(held[0] == columns[u], second)
                tile = right_at(k % rows, jnp.where(second, 1, 0))
                wide.append(jnp.where(found, tile, jnp.zeros_like(tile)))
            deep.append(jnp.concatenate(wide, axis=1))
        weights = jnp.concatenate(deep, axis=0)
        factor = jnp.concatenate([left_at(i, s) for s in range(KP)], axis=1)
        return jnp.dot(factor, weights, preferred_element_type=jnp.float32)

    def tiles_of(ref, offset):
        return lambda i, s: ref[i, (offset + HALF) * KP + s]

    def chunk_of(ref, end):
        return lambda i, s: ref[end, i, s]

    def own_terms(left, right, column):
        def step(n, carry):
            for q in range(UNROLL):
                i = n * UNROLL + q
                acc[column + HALF, i] = term(i, 0, 0, column, tiles_of(left, 0), tiles_of(right, column))
            return carry

        lax.fori_loop(0, rows // UNROLL, step, 0)

    def group_terms(left, buffer, group):
        distance, column = group
        per = rows // UNROLL

        def step(n, carry):
            end = n // per
            sign = 1 - 2 * end
            middle, here = sign * distance, sign * column
            for q in range(UNROLL):
                i = (n % per) * UNROLL + q
                acc[here + HALF, i] += term(i, 0, middle, here, tiles_of(left, middle), chunk_of(buffer, end))
            return carry

        lax.fori_loop(0, 2 * per, step, 0)

    def mix(x_tile, total):
        tile = total.astype(jnp.bfloat16)
        return tile, coef[1] * x_tile.astype(jnp.float32) + coef[2] * tile.astype(jnp.float32)

    def form(group):
        distance, column = group
        per = rows // 2

        def step(n, carry):
            end = n // per
            sign = 1 - 2 * end
            for q in range(2):
                i = (n % per) * 2 + q
                total = None
                for middle in range(distance - HALF, column + HALF + 1):
                    left_at = chunk_of(arrived[0, (distance, middle)], end)
                    if middle > 0:
                        right_at = chunk_of(arrived[0, (middle, column)], end)
                    elif middle < 0:
                        right_at = chunk_of(arrived[0, (-middle, -column)], 1 - end)
                    else:
                        right_at = tiles_of(xv, sign * column)
                    product = term(i, sign * distance, sign * middle, sign * column, left_at, right_at)
                    total = product if total is None else total + product
                for u in range(KP):
                    x_tile = arrived[0, group][end, i, u]
                    formed[group][end, i, u] = mix(x_tile, total[:, u * side : (u + 1) * side])[1].astype(jnp.bfloat16)
            return carry

        lax.fori_loop(0, 2 * per, step, 0)

    def settle(column):
        def step(i, carry):
            total = acc[column + HALF, i]
            for u in range(KP):
                slot = (column + HALF) * KP + u
                tile, mixed = mix(xv[i, slot], total[:, u * side : (u + 1) * side])
                sv[i, slot] = tile
                if slot == HALF * KP:
                    down = lax.broadcasted_iota(jnp.int32, (side, side), 0)
                    across = lax.broadcasted_iota(jnp.int32, (side, side), 1)
                    mixed = mixed + jnp.where(down == across, coef[0], 0.0)
                bv[i, slot] = mixed.astype(jnp.bfloat16)
            return carry

        lax.fori_loop(0, rows, step, 0)
        own_terms(gv, bv, column)
        put(0, column, sv, squared_hbm)

    def put(which, column, source, target):
        slots = pl.ds((column + HALF) * KP, KP)
        copy = pltpu.make_async_copy(source.at[:, slots], target.at[:, slots], out_sem.at[which * SPREAD + column + HALF])
        copy.start()
        outs.append(copy)

    def finish(column):
        def step(i, carry):
            total = acc[column + HALF, i]
            for u in range(KP):
                rv[i, (column + HALF) * KP + u] = total[:, u * side : (u + 1) * side].astype(jnp.bfloat16)
            return carry

        lax.fori_loop(0, rows, step, 0)
        put(1, column, rv, result_hbm)

    loads[0].wait()
    for group in ORDER[0][:4]:
        start(0, group)
    for column in range(-HALF, HALF + 1):
        own_terms(xv, xv, column)
    loads[1].wait()
    for group in ORDER[0][:4]:
        onward = (group[0] + 1, group[1] + 1)
        arrive(0, group, onward if onward in ORDER[0] else None)
        group_terms(xv, arrived[0, group], group)
    form((1, -1))
    arrive(0, (2, 0))
    group_terms(xv, arrived[0, (2, 0)], (2, 0))
    settle(0)
    start(1, (1, 1))
    form((1, 0))
    start(1, (2, 1))
    arrive(0, (2, 1))
    group_terms(xv, arrived[0, (2, 1)], (2, 1))
    settle(1)
    settle(-1)
    start(1, (1, 2))
    arrive(0, (2, 2))
    group_terms(xv, arrived[0, (2, 2)], (2, 2))
    settle(2)
    settle(-2)
    form((2, 0))
    arrive(1, (1, 1), (2, 2))
    for group in FORMED:
        group_terms(gv, formed[group], group)
    finish(0)
    group_terms(gv, arrived[1, (1, 1)], (1, 1))
    arrive(1, (2, 1))
    group_terms(gv, arrived[1, (2, 1)], (2, 1))
    finish(1)
    finish(-1)
    arrive(1, (1, 2))
    group_terms(gv, arrived[1, (1, 2)], (1, 2))
    arrive(1, (2, 2))
    group_terms(gv, arrived[1, (2, 2)], (2, 2))
    finish(2)
    finish(-2)
    for copy in outs:
        copy.wait()
    for copy in sends:
        copy.wait_send()


def solution(mesh):
    panels = mesh.shape["rows"]
    copies = mesh.shape["rep"] // 2

    def local(x_tiles, giant_tiles, coeffs, pattern):
        rows, slots, side, _ = x_tiles.shape
        tiles = pltpu.VMEM(x_tiles.shape, jnp.bfloat16)
        chunk = pltpu.VMEM((2, rows, KP, side, side), jnp.bfloat16)
        moves = 2 * len(MOVES)
        outs = jax.ShapeDtypeStruct(x_tiles.shape, jnp.bfloat16)
        return pl.pallas_call(
            functools.partial(kernel, panels, 4, copies),
            out_shape=(outs, outs),
            in_specs=[
                pl.BlockSpec(memory_space=pltpu.SMEM),
                pl.BlockSpec(memory_space=pltpu.SMEM),
                pl.BlockSpec(memory_space=pl.ANY),
                pl.BlockSpec(memory_space=pl.ANY),
            ],
            out_specs=(pl.BlockSpec(memory_space=pl.ANY), pl.BlockSpec(memory_space=pl.ANY)),
            scratch_shapes=[
                tiles,
                tiles,
                tiles,
                tiles,
                tiles,
                pltpu.VMEM((SPREAD, rows, side, KP * side), jnp.float32),
                *[chunk for _ in MOVES + list(FORMED)],
                pltpu.SemaphoreType.DMA((2,)),
                pltpu.SemaphoreType.DMA((2 * SPREAD,)),
                pltpu.SemaphoreType.DMA((moves,)),
                pltpu.SemaphoreType.DMA((moves,)),
                pltpu.SemaphoreType.DMA((moves,)),
                pltpu.SemaphoreType.DMA((moves,)),
            ],
            compiler_params=pltpu.CompilerParams(
                collective_id=0, has_side_effects=True, vmem_limit_bytes=60 * 1024 * 1024
            ),
        )(pattern.reshape(-1), coeffs, x_tiles, giant_tiles)

    return jax.shard_map(
        local,
        mesh=mesh,
        in_specs=(P("rows", None, None, None), P("rows", None, None, None), P(), P()),
        out_specs=(P("rows", None, None, None), P("rows", None, None, None)),
        check_vma=False,
    )
```

```python
import functools

import jax
import jax.numpy as jnp
from jax import lax
from jax.experimental import pallas as pl
from jax.experimental.pallas import tpu as pltpu
from jax.sharding import PartitionSpec as P

HALF = 2
KP = 2
SPREAD = 2 * HALF + 1
UNROLL = 4
MESH = pl.DeviceIdType.MESH

ORDER = (
    ((1, -1), (1, 0), (1, 1), (1, 2), (2, 0), (2, 1), (2, 2)),
    ((1, 1), (2, 1), (1, 2), (2, 2)),
)
FORMED = ((1, -1), (1, 0), (2, 0))
MOVES = [(phase, group) for phase in (0, 1) for group in ORDER[phase]]
SHARED = MOVES + [("formed", group) for group in FORMED]


def kernel(panels, run, copies, pat, coef, x_hbm, g_hbm, sv, rv, *scratch):
    xv, gv, bv, acc = scratch[:4]
    arrived = dict(zip(SHARED, scratch[4:]))
    formed = {group: arrived["formed", group] for group in FORMED}
    load_sem, send_sem, recv_sem, push_sem, pull_sem = scratch[-5:]
    rows = xv.shape[0]
    side = xv.shape[2]
    half = rows // 2
    panel = lax.axis_index("rows")
    rep = lax.axis_index("rep")
    core = rep % 2
    zone = rep // 2
    place = panel % run
    if copies > 1:
        zone_up = jnp.where(place == run - 1, 1 - zone, zone)
        zone_down = jnp.where(place == 0, 1 - zone, zone)
    else:
        zone_up = zone
        zone_down = zone
    above = ((panel + 1) % panels, zone_up * 2 + core)
    below = ((panel + panels - 1) % panels, zone_down * 2 + core)
    partner = (panel, zone * 2 + 1 - core)

    loads = [pltpu.make_async_copy(x_hbm, xv, load_sem.at[0]), pltpu.make_async_copy(g_hbm, gv, load_sem.at[1])]
    for load in loads:
        load.start()

    barrier = pltpu.get_barrier_semaphore()
    for other in (above, below, partner):
        pl.semaphore_signal(barrier, inc=1, device_id=other, device_id_type=MESH)
    pl.semaphore_wait(barrier, 3)

    mine = (xv, bv)
    my_half = pl.ds(core * half, half)
    sends = []

    def hop(phase, group, end):
        distance, column = group
        if distance == 1:
            slots = (1 - 2 * end) * (column - distance) + HALF
            source = mine[phase].at[my_half, pl.ds(slots * KP, KP)]
        else:
            passed = (distance - 1, column - 1)
            held = formed[passed] if phase and passed in FORMED else arrived[phase, passed]
            source = held.at[end, my_half]
        index = MOVES.index((phase, group)) * 2 + end
        return pltpu.make_async_remote_copy(
            src_ref=source,
            dst_ref=arrived[phase, group].at[end, my_half],
            send_sem=send_sem.at[index],
            recv_sem=recv_sem.at[index],
            device_id=above if end else below,
            device_id_type=MESH,
        )

    def push(key, end):
        index = SHARED.index(key) * 2 + end
        block = arrived[key].at[end, my_half]
        return pltpu.make_async_remote_copy(
            src_ref=block,
            dst_ref=block,
            send_sem=push_sem.at[index],
            recv_sem=pull_sem.at[index],
            device_id=partner,
            device_id_type=MESH,
        )

    def start(phase, group):
        for end in (0, 1):
            copy = hop(phase, group, end)
            copy.start()
            sends.append(copy)

    def share(key):
        for end in (0, 1):
            copy = push(key, end)
            copy.start()
            sends.append(copy)

    def arrive(phase, group):
        for end in (0, 1):
            hop(phase, group, end).wait_recv()
        onward = (group[0] + 1, group[1] + 1)
        if onward in ORDER[phase] and not (phase and group in FORMED):
            start(phase, onward)
        share((phase, group))

    def whole(key):
        for end in (0, 1):
            push(key, end).wait_recv()

    def term(i, row, middle, column, left_at, right_at):
        at = (panel + row + panels) % panels * rows + i
        first = (middle - row + HALF) * KP
        wanted = (column - row + HALF) * KP
        offered = (column - middle + HALF) * KP
        columns = [pat[wanted + u, at] for u in range(KP)]
        deep = []
        for s in range(KP):
            k = pat[first + s, at]
            held = [pat[offered + t, k] for t in range(KP)]
            wide = []
            for u in range(KP):
                second = held[1] == columns[u]
                found = jnp.logical_or(held[0] == columns[u], second)
                tile = right_at(k % rows, jnp.where(second, 1, 0))
                wide.append(jnp.where(found, tile, jnp.zeros_like(tile)))
            deep.append(jnp.concatenate(wide, axis=1))
        weights = jnp.concatenate(deep, axis=0)
        factor = jnp.concatenate([left_at(i, s) for s in range(KP)], axis=1)
        return jnp.dot(factor, weights, preferred_element_type=jnp.float32)

    def tiles_of(ref, offset):
        return lambda i, s: ref[i, (offset + HALF) * KP + s]

    def chunk_of(ref, end):
        return lambda i, s: ref[end, i, s]

    def own_terms(left, right, column):
        def step(n, carry):
            for q in range(UNROLL):
                i = n * UNROLL + q
                acc[column + HALF, i] = term(i, 0, 0, column, tiles_of(left, 0), tiles_of(right, column))
            return carry

        lax.fori_loop(0, rows // UNROLL, step, 0)

    def group_terms(left, buffer, group):
        distance, column = group
        per = rows // UNROLL

        def step(n, carry):
            end = n // per
            sign = 1 - 2 * end
            middle, here = sign * distance, sign * column
            for q in range(UNROLL):
                i = (n % per) * UNROLL + q
                acc[here + HALF, i] += term(i, 0, middle, here, tiles_of(left, middle), chunk_of(buffer, end))
            return carry

        lax.fori_loop(0, 2 * per, step, 0)

    def mix(x_tile, total):
        tile = total.astype(jnp.bfloat16)
        return tile, coef[1] * x_tile.astype(jnp.float32) + coef[2] * tile.astype(jnp.float32)

    def form(group):
        distance, column = group
        per = half // 2

        def step(n, carry):
            end = n // per
            sign = 1 - 2 * end
            for q in range(2):
                i = core * half + (n % per) * 2 + q
                total = None
                for middle in range(distance - HALF, column + HALF + 1):
                    left_at = chunk_of(arrived[0, (distance, middle)], end)
                    if middle > 0:
                        right_at = chunk_of(arrived[0, (middle, column)], end)
                    elif middle < 0:
                        right_at = chunk_of(arrived[0, (-middle, -column)], 1 - end)
                    else:
                        right_at = tiles_of(xv, sign * column)
                    product = term(i, sign * distance, sign * middle, sign * column, left_at, right_at)
                    total = product if total is None else total + product
                for u in range(KP):
                    x_tile = arrived[0, group][end, i, u]
                    formed[group][end, i, u] = mix(x_tile, total[:, u * side : (u + 1) * side])[1].astype(jnp.bfloat16)
            return carry

        lax.fori_loop(0, 2 * per, step, 0)
        share(("formed", group))

    def settle(column):
        def step(i, carry):
            total = acc[column + HALF, i]
            for u in range(KP):
                slot = (column + HALF) * KP + u
                tile, mixed = mix(xv[i, slot], total[:, u * side : (u + 1) * side])
                sv[i, slot] = tile
                if slot == HALF * KP:
                    down = lax.broadcasted_iota(jnp.int32, (side, side), 0)
                    across = lax.broadcasted_iota(jnp.int32, (side, side), 1)
                    mixed = mixed + jnp.where(down == across, coef[0], 0.0)
                bv[i, slot] = mixed.astype(jnp.bfloat16)
            return carry

        lax.fori_loop(0, rows, step, 0)
        own_terms(gv, bv, column)

    def finish(column):
        def step(i, carry):
            total = acc[column + HALF, i]
            for u in range(KP):
                rv[i, (column + HALF) * KP + u] = total[:, u * side : (u + 1) * side].astype(jnp.bfloat16)
            return carry

        lax.fori_loop(0, rows, step, 0)

    def add_x(group):
        whole((0, group))
        group_terms(xv, arrived[0, group], group)

    def add_baby(group):
        key = ("formed" if group in FORMED else 1, group)
        whole(key)
        group_terms(gv, arrived[key], group)

    loads[0].wait()
    for group in ORDER[0][:4]:
        start(0, group)
    for column in range(-HALF, HALF + 1):
        own_terms(xv, xv, column)
    loads[1].wait()
    for group in ORDER[0][:3]:
        arrive(0, group)
        add_x(group)
    form((1, -1))
    arrive(0, (1, 2))
    add_x((1, 2))
    arrive(0, (2, 0))
    add_x((2, 0))
    settle(0)
    start(1, (1, 1))
    form((1, 0))
    start(1, (2, 1))
    arrive(0, (2, 1))
    add_x((2, 1))
    settle(1)
    settle(-1)
    start(1, (1, 2))
    arrive(0, (2, 2))
    form((2, 0))
    add_x((2, 2))
    settle(2)
    settle(-2)
    add_baby((1, -1))
    arrive(1, (1, 1))
    add_baby((1, 0))
    add_baby((2, 0))
    finish(0)
    add_baby((1, 1))
    arrive(1, (2, 1))
    add_baby((2, 1))
    finish(1)
    finish(-1)
    arrive(1, (1, 2))
    add_baby((1, 2))
    arrive(1, (2, 2))
    add_baby((2, 2))
    finish(2)
    finish(-2)
    for copy in sends:
        copy.wait_send()


def write(squared, result, squared_hbm, result_hbm, sem):
    copies = [pltpu.make_async_copy(squared, squared_hbm, sem.at[0]), pltpu.make_async_copy(result, result_hbm, sem.at[1])]
    for copy in copies:
        copy.start()
    for copy in copies:
        copy.wait()


def solution(mesh):
    panels = mesh.shape["rows"]
    copies = mesh.shape["rep"] // 2

    def local(x_tiles, giant_tiles, coeffs, pattern):
        rows, slots, side, _ = x_tiles.shape
        tiles = pltpu.VMEM(x_tiles.shape, jnp.bfloat16)
        chunk = pltpu.VMEM((2, rows, KP, side, side), jnp.bfloat16)
        outs = jax.ShapeDtypeStruct(x_tiles.shape, jnp.bfloat16)
        held = pl.pallas_call(
            functools.partial(kernel, panels, 4, copies),
            out_shape=(outs, outs),
            in_specs=[
                pl.BlockSpec(memory_space=pltpu.SMEM),
                pl.BlockSpec(memory_space=pltpu.SMEM),
                pl.BlockSpec(memory_space=pltpu.HBM),
                pl.BlockSpec(memory_space=pltpu.HBM),
            ],
            out_specs=(pl.BlockSpec(memory_space=pltpu.VMEM), pl.BlockSpec(memory_space=pltpu.VMEM)),
            scratch_shapes=[
                tiles,
                tiles,
                tiles,
                pltpu.VMEM((SPREAD, rows, side, KP * side), jnp.float32),
                *[chunk for _ in SHARED],
                pltpu.SemaphoreType.DMA((2,)),
                pltpu.SemaphoreType.DMA((2 * len(MOVES),)),
                pltpu.SemaphoreType.DMA((2 * len(MOVES),)),
                pltpu.SemaphoreType.DMA((2 * len(SHARED),)),
                pltpu.SemaphoreType.DMA((2 * len(SHARED),)),
            ],
            compiler_params=pltpu.CompilerParams(
                collective_id=0, has_side_effects=True, vmem_limit_bytes=47 * 1024 * 1024
            ),
        )(pattern.T, coeffs, x_tiles, giant_tiles)
        return pl.pallas_call(
            write,
            out_shape=(outs, outs),
            in_specs=[pl.BlockSpec(memory_space=pltpu.VMEM)] * 2,
            out_specs=(pl.BlockSpec(memory_space=pltpu.HBM), pl.BlockSpec(memory_space=pltpu.HBM)),
            scratch_shapes=[pltpu.SemaphoreType.DMA((2,))],
            compiler_params=pltpu.CompilerParams(vmem_limit_bytes=8 * 1024 * 1024),
        )(*held)

    return jax.shard_map(
        local,
        mesh=mesh,
        in_specs=(P("rows", None, None, None), P("rows", None, None, None), P(), P()),
        out_specs=(P("rows", None, None, None), P("rows", None, None, None)),
        check_vma=False,
    )
```

```python
import functools

import jax
import jax.numpy as jnp
from jax import lax
from jax.experimental import pallas as pl
from jax.experimental.pallas import tpu as pltpu
from jax.sharding import PartitionSpec as P

HALF = 2
KP = 2
SPREAD = 2 * HALF + 1
UNROLL = 8
MESH = pl.DeviceIdType.MESH

ORDER = (
    ((1, -1), (1, 0), (1, 1), (1, 2), (2, 0), (2, 1), (2, 2)),
    ((1, 1), (2, 1), (1, 2), (2, 2)),
)
FORMED = ((1, -1), (1, 0), (2, 0))
MOVES = [(phase, group) for phase in (0, 1) for group in ORDER[phase]]
SHARED = MOVES + [("formed", group) for group in FORMED]


def kernel(panels, run, copies, pat_hbm, coef_hbm, x_hbm, g_hbm, sv, rv, pat, coef, *scratch):
    xv, gv, bv, acc = scratch[:4]
    arrived = dict(zip(SHARED, scratch[4:]))
    formed = {group: arrived["formed", group] for group in FORMED}
    load_sem, send_sem, recv_sem, push_sem, pull_sem = scratch[-5:]
    rows = xv.shape[0]
    side = xv.shape[2]
    half = rows // 2
    panel = lax.axis_index("rows")
    rep = lax.axis_index("rep")
    core = rep % 2
    zone = rep // 2
    place = panel % run
    if copies > 1:
        zone_up = jnp.where(place == run - 1, 1 - zone, zone)
        zone_down = jnp.where(place == 0, 1 - zone, zone)
    else:
        zone_up = zone
        zone_down = zone
    above = ((panel + 1) % panels, zone_up * 2 + core)
    below = ((panel + panels - 1) % panels, zone_down * 2 + core)
    partner = (panel, zone * 2 + 1 - core)

    barrier = pltpu.get_barrier_semaphore()
    for other in (above, below, partner):
        pl.semaphore_signal(barrier, inc=1, device_id=other, device_id_type=MESH)
    pairs = ((pat_hbm, pat), (coef_hbm, coef), (x_hbm, xv), (g_hbm, gv))
    loads = [pltpu.make_async_copy(source, target, load_sem.at[n]) for n, (source, target) in enumerate(pairs)]
    for load in loads:
        load.start()
    pl.semaphore_wait(barrier, 3)

    mine = (x_hbm, bv)
    my_half = pl.ds(core * half, half)
    sends = []

    def hop(phase, group, end):
        distance, column = group
        if distance == 1:
            slots = (1 - 2 * end) * (column - distance) + HALF
            source = mine[phase].at[my_half, pl.ds(slots * KP, KP)]
        else:
            passed = (distance - 1, column - 1)
            held = formed[passed] if phase and passed in FORMED else arrived[phase, passed]
            source = held.at[end, my_half]
        index = MOVES.index((phase, group)) * 2 + end
        return pltpu.make_async_remote_copy(
            src_ref=source,
            dst_ref=arrived[phase, group].at[end, my_half],
            send_sem=send_sem.at[index],
            recv_sem=recv_sem.at[index],
            device_id=above if end else below,
            device_id_type=MESH,
        )

    def push(key, end):
        index = SHARED.index(key) * 2 + end
        block = arrived[key].at[end, my_half]
        return pltpu.make_async_remote_copy(
            src_ref=block,
            dst_ref=block,
            send_sem=push_sem.at[index],
            recv_sem=pull_sem.at[index],
            device_id=partner,
            device_id_type=MESH,
        )

    def start(phase, group):
        for end in (0, 1):
            copy = hop(phase, group, end)
            copy.start()
            sends.append(copy)

    def share(key):
        for end in (0, 1):
            copy = push(key, end)
            copy.start()
            sends.append(copy)

    def arrive(phase, group):
        for end in (0, 1):
            hop(phase, group, end).wait_recv()
        onward = (group[0] + 1, group[1] + 1)
        if onward in ORDER[phase] and not (phase and group in FORMED):
            start(phase, onward)
        share((phase, group))

    def whole(key):
        for end in (0, 1):
            push(key, end).wait_recv()

    def term(i, row, middle, column, left_at, right_at):
        at = (panel + row + panels) % panels * rows + i
        first = (middle - row + HALF) * KP
        wanted = (column - row + HALF) * KP
        offered = (column - middle + HALF) * KP
        columns = [pat[wanted + u, at] for u in range(KP)]
        deep = []
        for s in range(KP):
            k = pat[first + s, at]
            held = [pat[offered + t, k] for t in range(KP)]
            wide = []
            for u in range(KP):
                second = held[1] == columns[u]
                found = jnp.logical_or(held[0] == columns[u], second)
                tile = right_at(k % rows, jnp.where(second, 1, 0))
                wide.append(jnp.where(found, tile, jnp.zeros_like(tile)))
            deep.append(jnp.concatenate(wide, axis=1))
        weights = jnp.concatenate(deep, axis=0)
        factor = jnp.concatenate([left_at(i, s) for s in range(KP)], axis=1)
        return jnp.dot(factor, weights, preferred_element_type=jnp.float32)

    def tiles_of(ref, offset):
        return lambda i, s: ref[i, (offset + HALF) * KP + s]

    def chunk_of(ref, end):
        return lambda i, s: ref[end, i, s]

    def own_terms(left, right, column):
        def step(n, carry):
            for q in range(UNROLL):
                i = n * UNROLL + q
                acc[column + HALF, i] = term(i, 0, 0, column, tiles_of(left, 0), tiles_of(right, column))
            return carry

        lax.fori_loop(0, rows // UNROLL, step, 0)

    def group_terms(left, buffer, group, last=False):
        distance, column = group
        per = rows // UNROLL

        def step(n, carry):
            end = n // per
            sign = 1 - 2 * end
            middle, here = sign * distance, sign * column
            for q in range(UNROLL):
                i = (n % per) * UNROLL + q
                total = acc[here + HALF, i] + term(i, 0, middle, here, tiles_of(left, middle), chunk_of(buffer, end))
                if last:
                    for u in range(KP):
                        rv[i, (here + HALF) * KP + u] = total[:, u * side : (u + 1) * side].astype(jnp.bfloat16)
                else:
                    acc[here + HALF, i] = total
            return carry

        lax.fori_loop(0, 2 * per, step, 0)

    def mix(x_tile, total):
        tile = total.astype(jnp.bfloat16)
        return tile, coef[1] * x_tile.astype(jnp.float32) + coef[2] * tile.astype(jnp.float32)

    def form(group):
        distance, column = group
        per = half // 2

        def step(n, carry):
            end = n // per
            sign = 1 - 2 * end
            for q in range(2):
                i = core * half + (n % per) * 2 + q
                total = None
                for middle in range(distance - HALF, column + HALF + 1):
                    left_at = chunk_of(arrived[0, (distance, middle)], end)
                    if middle > 0:
                        right_at = chunk_of(arrived[0, (middle, column)], end)
                    elif middle < 0:
                        right_at = chunk_of(arrived[0, (-middle, -column)], 1 - end)
                    else:
                        right_at = tiles_of(xv, sign * column)
                    product = term(i, sign * distance, sign * middle, sign * column, left_at, right_at)
                    total = product if total is None else total + product
                for u in range(KP):
                    x_tile = arrived[0, group][end, i, u]
                    formed[group][end, i, u] = mix(x_tile, total[:, u * side : (u + 1) * side])[1].astype(jnp.bfloat16)
            return carry

        lax.fori_loop(0, 2 * per, step, 0)
        share(("formed", group))

    def settle(column):
        def step(i, carry):
            total = acc[column + HALF, i]
            for u in range(KP):
                slot = (column + HALF) * KP + u
                tile, mixed = mix(xv[i, slot], total[:, u * side : (u + 1) * side])
                sv[i, slot] = tile
                if slot == HALF * KP:
                    down = lax.broadcasted_iota(jnp.int32, (side, side), 0)
                    across = lax.broadcasted_iota(jnp.int32, (side, side), 1)
                    mixed = mixed + jnp.where(down == across, coef[0], 0.0)
                bv[i, slot] = mixed.astype(jnp.bfloat16)
            return carry

        lax.fori_loop(0, rows, step, 0)
        own_terms(gv, bv, column)

    def finish(column):
        def step(i, carry):
            total = acc[column + HALF, i]
            for u in range(KP):
                rv[i, (column + HALF) * KP + u] = total[:, u * side : (u + 1) * side].astype(jnp.bfloat16)
            return carry

        lax.fori_loop(0, rows, step, 0)

    def add_x(group):
        whole((0, group))
        group_terms(xv, arrived[0, group], group)

    def add_baby(group, last=False):
        key = ("formed" if group in FORMED else 1, group)
        whole(key)
        group_terms(gv, arrived[key], group, last)

    for group in ORDER[0][:4]:
        start(0, group)
    for load in loads:
        load.wait()
    for column in range(-HALF, HALF + 1):
        own_terms(xv, xv, column)
    for group in ORDER[0][:3]:
        arrive(0, group)
        add_x(group)
    form((1, -1))
    arrive(0, (1, 2))
    add_x((1, 2))
    arrive(0, (2, 0))
    add_x((2, 0))
    settle(0)
    start(1, (1, 1))
    form((1, 0))
    start(1, (2, 1))
    arrive(0, (2, 1))
    add_x((2, 1))
    settle(1)
    settle(-1)
    start(1, (1, 2))
    arrive(0, (2, 2))
    form((2, 0))
    add_x((2, 2))
    settle(2)
    settle(-2)
    add_baby((1, -1))
    arrive(1, (1, 1))
    add_baby((1, 0))
    add_baby((1, 1))
    add_baby((2, 0))
    finish(0)
    arrive(1, (2, 1))
    add_baby((2, 1), last=True)
    arrive(1, (1, 2))
    add_baby((1, 2))
    arrive(1, (2, 2))
    add_baby((2, 2), last=True)
    for copy in sends:
        copy.wait_send()


def write(squared, result, squared_hbm, result_hbm, sem):
    copies = [pltpu.make_async_copy(squared, squared_hbm, sem.at[0]), pltpu.make_async_copy(result, result_hbm, sem.at[1])]
    for copy in copies:
        copy.start()
    for copy in copies:
        copy.wait()


def solution(mesh):
    panels = mesh.shape["rows"]
    copies = mesh.shape["rep"] // 2

    def local(x_tiles, giant_tiles, coeffs, pattern):
        rows, slots, side, _ = x_tiles.shape
        tiles = pltpu.VMEM(x_tiles.shape, jnp.bfloat16)
        chunk = pltpu.VMEM((2, rows, KP, side, side), jnp.bfloat16)
        outs = jax.ShapeDtypeStruct(x_tiles.shape, jnp.bfloat16)
        held = pl.pallas_call(
            functools.partial(kernel, panels, 4, copies),
            out_shape=(outs, outs),
            in_specs=[
                pl.BlockSpec(memory_space=pltpu.HBM),
                pl.BlockSpec(memory_space=pltpu.HBM),
                pl.BlockSpec(memory_space=pltpu.HBM),
                pl.BlockSpec(memory_space=pltpu.HBM),
            ],
            out_specs=(pl.BlockSpec(memory_space=pltpu.VMEM), pl.BlockSpec(memory_space=pltpu.VMEM)),
            scratch_shapes=[
                pltpu.SMEM((slots, pattern.shape[0]), jnp.int32),
                pltpu.SMEM(coeffs.shape, jnp.float32),
                tiles,
                tiles,
                tiles,
                pltpu.VMEM((SPREAD, rows, side, KP * side), jnp.float32),
                *[chunk for _ in SHARED],
                pltpu.SemaphoreType.DMA((4,)),
                pltpu.SemaphoreType.DMA((2 * len(MOVES),)),
                pltpu.SemaphoreType.DMA((2 * len(MOVES),)),
                pltpu.SemaphoreType.DMA((2 * len(SHARED),)),
                pltpu.SemaphoreType.DMA((2 * len(SHARED),)),
            ],
            compiler_params=pltpu.CompilerParams(
                collective_id=0, has_side_effects=True, vmem_limit_bytes=47 * 1024 * 1024
            ),
        )(*(pltpu.with_memory_space_constraint(value, pltpu.HBM) for value in (pattern.T, coeffs, x_tiles, giant_tiles)))
        return pl.pallas_call(
            write,
            out_shape=(outs, outs),
            in_specs=[pl.BlockSpec(memory_space=pltpu.VMEM)] * 2,
            out_specs=(pl.BlockSpec(memory_space=pltpu.HBM), pl.BlockSpec(memory_space=pltpu.HBM)),
            scratch_shapes=[pltpu.SemaphoreType.DMA((2,))],
            compiler_params=pltpu.CompilerParams(vmem_limit_bytes=8 * 1024 * 1024),
        )(*held)

    return jax.shard_map(
        local,
        mesh=mesh,
        in_specs=(P("rows", None, None, None), P("rows", None, None, None), P(), P()),
        out_specs=(P("rows", None, None, None), P("rows", None, None, None)),
        check_vma=False,
    )
```

```python
import functools

import jax
import jax.numpy as jnp
from jax import lax
from jax.experimental import pallas as pl
from jax.experimental.pallas import tpu as pltpu
from jax.sharding import PartitionSpec as P

HALF = 2
KP = 2
SPREAD = 2 * HALF + 1
UNROLL = 8
MESH = pl.DeviceIdType.MESH

ORDER = (
    ((1, -1), (1, 0), (1, 1), (1, 2), (2, 0), (2, 1), (2, 2)),
    ((1, 1), (2, 1), (1, 2), (2, 2)),
)
FORMED = ((1, -1), (1, 0), (2, 0))
MOVES = [(phase, group) for phase in (0, 1) for group in ORDER[phase]]
SHARED = MOVES + [("formed", group) for group in FORMED]


def kernel(panels, run, copies, pat_hbm, coef_hbm, x_hbm, g_hbm, sv, rv, pat, coef, *scratch):
    xv, gv, bv, acc = scratch[:4]
    arrived = dict(zip(SHARED, scratch[4:]))
    formed = {group: arrived["formed", group] for group in FORMED}
    load_sem, send_sem, recv_sem, push_sem, pull_sem = scratch[-5:]
    rows = xv.shape[0]
    side = xv.shape[2]
    half = rows // 2
    panel = lax.axis_index("rows")
    rep = lax.axis_index("rep")
    core = rep % 2
    zone = rep // 2
    place = panel % run
    if copies > 1:
        zone_up = jnp.where(place == run - 1, 1 - zone, zone)
        zone_down = jnp.where(place == 0, 1 - zone, zone)
    else:
        zone_up = zone
        zone_down = zone
    above = ((panel + 1) % panels, zone_up * 2 + core)
    below = ((panel + panels - 1) % panels, zone_down * 2 + core)
    partner = (panel, zone * 2 + 1 - core)

    barrier = pltpu.get_barrier_semaphore()
    for other in (above, below, partner):
        pl.semaphore_signal(barrier, inc=1, device_id=other, device_id_type=MESH)
    pairs = ((pat_hbm, pat), (coef_hbm, coef), (x_hbm, xv), (g_hbm, gv))
    loads = [pltpu.make_async_copy(source, target, load_sem.at[n]) for n, (source, target) in enumerate(pairs)]
    pl.semaphore_wait(barrier, 3)

    mine = (x_hbm, bv)
    my_half = pl.ds(core * half, half)
    sends = []

    def hop(phase, group, end):
        distance, column = group
        if distance == 1:
            slots = (1 - 2 * end) * (column - distance) + HALF
            source = mine[phase].at[my_half, pl.ds(slots * KP, KP)]
        else:
            passed = (distance - 1, column - 1)
            held = formed[passed] if phase and passed in FORMED else arrived[phase, passed]
            source = held.at[end, my_half]
        index = MOVES.index((phase, group)) * 2 + end
        return pltpu.make_async_remote_copy(
            src_ref=source,
            dst_ref=arrived[phase, group].at[end, my_half],
            send_sem=send_sem.at[index],
            recv_sem=recv_sem.at[index],
            device_id=above if end else below,
            device_id_type=MESH,
        )

    def push(key, end):
        index = SHARED.index(key) * 2 + end
        block = arrived[key].at[end, my_half]
        return pltpu.make_async_remote_copy(
            src_ref=block,
            dst_ref=block,
            send_sem=push_sem.at[index],
            recv_sem=pull_sem.at[index],
            device_id=partner,
            device_id_type=MESH,
        )

    def go(copy):
        copy.start()
        sends.append(copy)

    def start(phase, group):
        for end in (0, 1):
            go(hop(phase, group, end))

    def share(key):
        for end in (0, 1):
            go(push(key, end))

    def arrive(phase, group):
        onward = (group[0] + 1, group[1] + 1)
        for end in (0, 1):
            hop(phase, group, end).wait_recv()
            if onward in ORDER[phase] and not (phase and group in FORMED):
                go(hop(phase, onward, end))
            go(push((phase, group), end))

    def whole(key):
        for end in (0, 1):
            push(key, end).wait_recv()

    def term(i, row, middle, column, left_at, right_at):
        at = (panel + row + panels) % panels * rows + i
        first = (middle - row + HALF) * KP
        wanted = (column - row + HALF) * KP
        offered = (column - middle + HALF) * KP
        columns = [pat[wanted + u, at] for u in range(KP)]
        deep = []
        for s in range(KP):
            k = pat[first + s, at]
            held = [pat[offered + t, k] for t in range(KP)]
            wide = []
            for u in range(KP):
                second = held[1] == columns[u]
                found = jnp.logical_or(held[0] == columns[u], second)
                tile = right_at(k % rows, jnp.where(second, 1, 0))
                wide.append(jnp.where(found, tile, jnp.zeros_like(tile)))
            deep.append(jnp.concatenate(wide, axis=1))
        weights = jnp.concatenate(deep, axis=0)
        factor = jnp.concatenate([left_at(i, s) for s in range(KP)], axis=1)
        return jnp.dot(factor, weights, preferred_element_type=jnp.float32)

    def tiles_of(ref, offset):
        return lambda i, s: ref[i, (offset + HALF) * KP + s]

    def chunk_of(ref, end):
        return lambda i, s: ref[end, i, s]

    def own_terms(left, right, column):
        def step(n, carry):
            for q in range(UNROLL):
                i = n * UNROLL + q
                acc[column + HALF, i] = term(i, 0, 0, column, tiles_of(left, 0), tiles_of(right, column))
            return carry

        lax.fori_loop(0, rows // UNROLL, step, 0)

    def group_terms(left, buffer, group, last=False):
        distance, column = group
        per = rows // UNROLL

        def step(n, carry):
            end = n // per
            sign = 1 - 2 * end
            middle, here = sign * distance, sign * column
            for q in range(UNROLL):
                i = (n % per) * UNROLL + q
                total = acc[here + HALF, i] + term(i, 0, middle, here, tiles_of(left, middle), chunk_of(buffer, end))
                if last:
                    for u in range(KP):
                        rv[i, (here + HALF) * KP + u] = total[:, u * side : (u + 1) * side].astype(jnp.bfloat16)
                else:
                    acc[here + HALF, i] = total
            return carry

        lax.fori_loop(0, 2 * per, step, 0)

    def mix(x_tile, total):
        tile = total.astype(jnp.bfloat16)
        return tile, coef[1] * x_tile.astype(jnp.float32) + coef[2] * tile.astype(jnp.float32)

    def form(group):
        distance, column = group
        per = half // 2

        def step(n, carry):
            end = n // per
            sign = 1 - 2 * end
            for q in range(2):
                i = core * half + (n % per) * 2 + q
                total = None
                for middle in range(distance - HALF, column + HALF + 1):
                    left_at = chunk_of(arrived[0, (distance, middle)], end)
                    if middle > 0:
                        right_at = chunk_of(arrived[0, (middle, column)], end)
                    elif middle < 0:
                        right_at = chunk_of(arrived[0, (-middle, -column)], 1 - end)
                    else:
                        right_at = tiles_of(xv, sign * column)
                    product = term(i, sign * distance, sign * middle, sign * column, left_at, right_at)
                    total = product if total is None else total + product
                for u in range(KP):
                    x_tile = arrived[0, group][end, i, u]
                    formed[group][end, i, u] = mix(x_tile, total[:, u * side : (u + 1) * side])[1].astype(jnp.bfloat16)
            return carry

        lax.fori_loop(0, 2 * per, step, 0)
        share(("formed", group))

    def settle(column):
        def step(i, carry):
            total = acc[column + HALF, i]
            for u in range(KP):
                slot = (column + HALF) * KP + u
                tile, mixed = mix(xv[i, slot], total[:, u * side : (u + 1) * side])
                sv[i, slot] = tile
                if slot == HALF * KP:
                    down = lax.broadcasted_iota(jnp.int32, (side, side), 0)
                    across = lax.broadcasted_iota(jnp.int32, (side, side), 1)
                    mixed = mixed + jnp.where(down == across, coef[0], 0.0)
                bv[i, slot] = mixed.astype(jnp.bfloat16)
            return carry

        lax.fori_loop(0, rows, step, 0)
        own_terms(gv, bv, column)

    def finish(column):
        def step(i, carry):
            total = acc[column + HALF, i]
            for u in range(KP):
                rv[i, (column + HALF) * KP + u] = total[:, u * side : (u + 1) * side].astype(jnp.bfloat16)
            return carry

        lax.fori_loop(0, rows, step, 0)

    def add_x(group):
        whole((0, group))
        group_terms(xv, arrived[0, group], group)

    def add_baby(group, last=False):
        key = ("formed" if group in FORMED else 1, group)
        whole(key)
        group_terms(gv, arrived[key], group, last)

    for group in ORDER[0][:4]:
        start(0, group)
    for load in loads:
        load.start()
    for load in loads:
        load.wait()
    for column in range(-HALF, HALF + 1):
        own_terms(xv, xv, column)
    for group in ORDER[0][:3]:
        arrive(0, group)
        add_x(group)
    form((1, -1))
    arrive(0, (1, 2))
    add_x((1, 2))
    arrive(0, (2, 0))
    add_x((2, 0))
    settle(0)
    start(1, (1, 1))
    form((1, 0))
    start(1, (2, 1))
    arrive(0, (2, 1))
    add_x((2, 1))
    settle(1)
    settle(-1)
    start(1, (1, 2))
    arrive(0, (2, 2))
    form((2, 0))
    add_x((2, 2))
    settle(2)
    settle(-2)
    add_baby((1, -1))
    arrive(1, (1, 1))
    add_baby((1, 0))
    add_baby((1, 1))
    add_baby((2, 0))
    finish(0)
    arrive(1, (2, 1))
    add_baby((2, 1), last=True)
    arrive(1, (1, 2))
    add_baby((1, 2))
    arrive(1, (2, 2))
    add_baby((2, 2), last=True)
    for copy in sends:
        copy.wait_send()


def write(squared, result, squared_hbm, result_hbm, sem):
    copies = [pltpu.make_async_copy(squared, squared_hbm, sem.at[0]), pltpu.make_async_copy(result, result_hbm, sem.at[1])]
    for copy in copies:
        copy.start()
    for copy in copies:
        copy.wait()


def solution(mesh):
    panels = mesh.shape["rows"]
    copies = mesh.shape["rep"] // 2

    def local(x_tiles, giant_tiles, coeffs, pattern):
        rows, slots, side, _ = x_tiles.shape
        tiles = pltpu.VMEM(x_tiles.shape, jnp.bfloat16)
        chunk = pltpu.VMEM((2, rows, KP, side, side), jnp.bfloat16)
        outs = jax.ShapeDtypeStruct(x_tiles.shape, jnp.bfloat16)
        held = pl.pallas_call(
            functools.partial(kernel, panels, 4, copies),
            out_shape=(outs, outs),
            in_specs=[
                pl.BlockSpec(memory_space=pltpu.HBM),
                pl.BlockSpec(memory_space=pltpu.HBM),
                pl.BlockSpec(memory_space=pltpu.HBM),
                pl.BlockSpec(memory_space=pltpu.HBM),
            ],
            out_specs=(pl.BlockSpec(memory_space=pltpu.VMEM), pl.BlockSpec(memory_space=pltpu.VMEM)),
            scratch_shapes=[
                pltpu.SMEM((slots, pattern.shape[0]), jnp.int32),
                pltpu.SMEM(coeffs.shape, jnp.float32),
                tiles,
                tiles,
                tiles,
                pltpu.VMEM((SPREAD, rows, side, KP * side), jnp.float32),
                *[chunk for _ in SHARED],
                pltpu.SemaphoreType.DMA((4,)),
                pltpu.SemaphoreType.DMA((2 * len(MOVES),)),
                pltpu.SemaphoreType.DMA((2 * len(MOVES),)),
                pltpu.SemaphoreType.DMA((2 * len(SHARED),)),
                pltpu.SemaphoreType.DMA((2 * len(SHARED),)),
            ],
            compiler_params=pltpu.CompilerParams(
                collective_id=0, has_side_effects=True, vmem_limit_bytes=47 * 1024 * 1024
            ),
        )(*(pltpu.with_memory_space_constraint(value, pltpu.HBM) for value in (pattern.T, coeffs, x_tiles, giant_tiles)))
        return pl.pallas_call(
            write,
            out_shape=(outs, outs),
            in_specs=[pl.BlockSpec(memory_space=pltpu.VMEM)] * 2,
            out_specs=(pl.BlockSpec(memory_space=pltpu.HBM), pl.BlockSpec(memory_space=pltpu.HBM)),
            scratch_shapes=[pltpu.SemaphoreType.DMA((2,))],
            compiler_params=pltpu.CompilerParams(vmem_limit_bytes=8 * 1024 * 1024),
        )(*held)

    return jax.shard_map(
        local,
        mesh=mesh,
        in_specs=(P("rows", None, None, None), P("rows", None, None, None), P(), P()),
        out_specs=(P("rows", None, None, None), P("rows", None, None, None)),
        check_vma=False,
    )
```
